256 devices in a mesh: rep: 2 (over x_hi), px: 8 (over y, core), py: 16 (over z, x_lo).
Axes of the slice: x: 4 (x_hi: 2, x_lo: 2; x = x_hi * 2 + x_lo), y: 4, z: 8, core: 2. Of those that a mesh axis runs over, the one named last changes fastest.
Arguments:
- density: float32 [4, 128, 128, 128], P('rep', 'px', 'py'), parts along dimension 0, may hold values from -6 to 6
- kernel_factors: float32 [3, 89, 256], replicated, as said below
Outputs:
- potential: float32 [4, 128, 128, 128], P('rep', 'px', 'py'), parts along dimension 0
The draws below stay inside these ranges and needn't reach their ends.
There are 2 independent parts, one for each index of `rep`. The reference program is written for one: setup_inputs(seed, part) draws one part's arguments, and reference() takes and returns one part's arrays. A program takes and returns all parts, laid end to end along the dimension named above; an argument that names none is the same for every part. Nothing has to cross between parts.
Inputs may be any that keep to these rules, and one draw needn't show every extreme that they name: Each factor is even in its frequency, kernel_factors[d, g, k] = kernel_factors[d, g, 256 - k], and is zero at k = 128.
All inputs are finite; a program needn't handle non-finite values.
Results may differ from the reference program's by a relative error of at most 0.00005.
Values sent between devices are 32-bit elements; how exact they have to be, the bound alone decides.
A program may use at most 64 MiB of HBM per device.

```python
import math
import jax
import jax.numpy as jnp
from jax import lax

N = 128
G = 89
B = 2
M = 256


def draw_kernel_factors(key, part):
    first_key, second_key = jax.random.split(jax.random.fold_in(key, 7))
    widths = jnp.exp(jax.random.uniform(first_key, (G,), jnp.float32, math.log(0.05), math.log(50.0)))
    weights = 20.0 / G * jnp.exp(jax.random.uniform(second_key, (G,), jnp.float32, math.log(0.5), math.log(2.0)))
    frequency = jnp.arange(M, dtype=jnp.int32)
    wrapped = jnp.minimum(frequency, M - frequency).astype(jnp.float32)
    argument = (2.0 * math.pi * wrapped / M) ** 2
    inside = (wrapped < N).astype(jnp.float32)
    base = jnp.exp(-widths[:, None] * argument[None, :]) * inside[None, :]
    return jnp.stack([base * weights[:, None], base, base], 0).astype(jnp.float32)


def levels(stream_key, extent, cuts, smallest, high):
    gain, own = 1.0, jax.random.fold_in(stream_key, 6)
    for dim, blocks in cuts:
        draws = jnp.exp(jax.random.uniform(jax.random.fold_in(own, dim), (blocks,), jnp.float32, smallest / len(cuts), high / len(cuts)))
        gain = gain * jnp.repeat(draws, extent[dim] // blocks).reshape([-1 if axis == dim else 1 for axis in range(len(extent))])
    return gain


def centred(key, shape, spread, most, pieces=(), held_as=jnp.bfloat16):
    level = levels(key, shape, pieces, -0.22, 0.18) if pieces else 1.0
    entries = jax.random.normal(key, shape, jnp.float32) * spread * level
    return jnp.minimum(jnp.maximum(entries, -most), most).astype(held_as)


def setup_inputs(seed: int = 0, part: int = 0) -> dict:
    key_of = jax.random.split(jax.random.key(seed), 3)
    part_splits = jax.random.split(jax.random.fold_in(key_of[2], part), 3)
    return {
        "density": centred(part_splits[0], (B, N, N, N), 1.0, 6.0, ((1, 8), (2, 16)), jnp.float32),
        "kernel_factors": draw_kernel_factors(jax.random.fold_in(key_of[2], 71), part),
    }


def reference(density, kernel_factors):
    highest = lax.Precision.HIGHEST
    plane_xy = kernel_factors[0][:, :, None] * kernel_factors[1][:, None, :]
    kernel = jnp.einsum("gxy,gz->xyz", plane_xy, kernel_factors[2], precision=highest)

    def solve_one(replica):
        padded = jnp.pad(replica, ((0, M - N), (0, M - N), (0, M - N)))
        spectrum = jnp.fft.fftn(padded)
        potential_field = jnp.fft.ifftn(spectrum * kernel).real
        return potential_field[:N, :N, :N].astype(jnp.float32)

    return lax.map(solve_one, density)
```

```python
import functools

import jax
import jax.numpy as jnp
import numpy as np
from jax import lax
from jax.experimental import pallas as pl
from jax.experimental.pallas import tpu as pltpu
from jax.sharding import PartitionSpec as P

MESH = pl.DeviceIdType.MESH
N = 128
CHIPS = 64
ROWS_Y = 4
F32, BF16 = jnp.float32, jnp.bfloat16
ORDER = [int(v) + 1 for v in np.random.RandomState(1).permutation(CHIPS - 1)]


def pieces(table):
    table = np.asarray(table, np.float64).astype(np.float32)
    high = table.astype(BF16)
    low = (table - high.astype(np.float32)).astype(BF16)
    return high, low


def tables():
    k, n = np.arange(N), np.arange(N)
    angle = (k[:, None] * n[None, :] % (2 * N)) * (np.pi / N)
    cos, sin = np.cos(angle), np.sin(angle)
    weight = np.where(k == 0, 1.0, 2.0)[:, None] / (2 * N)
    by_owner = np.stack([cos, sin], 1).reshape(2, 2 * CHIPS, N)
    by_owner_back = np.stack([cos * weight, sin * weight], 1).reshape(2, 2 * CHIPS, N)
    plain = np.concatenate([cos, sin], 0)
    back = np.concatenate([cos * weight, sin * weight], 0)
    cells = np.arange(N).reshape(8, 16).T.reshape(-1)
    out = []
    high, low = pieces(by_owner)
    out.append(np.concatenate([high, high, low], 2))
    high, low = pieces(plain.T)
    out.append(np.concatenate([high, high, low], 0))
    high, low = pieces(plain[:, cells])
    out.append(np.concatenate([high, high, low], 1))
    high, low = pieces(back[:, cells].T)
    out.append(np.concatenate([high, low], 0))
    high, low = pieces(back)
    out.append(np.concatenate([high, low], 1))
    high, low = pieces(by_owner_back)
    out.append(np.concatenate([high, low], 2))
    return out


def split(value):
    high = value.astype(BF16)
    return high, (value - high.astype(F32)).astype(BF16)


def dot(a, b, dims=((1,), (0,))):
    return lax.dot_general(a, b, (dims, ((), ())), preferred_element_type=F32)


def swap(blocks):
    group = lax.broadcasted_iota(jnp.int32, (8, N), 1) // 8
    for bit in range(4):
        step = 1 << bit
        low = (group // step) % 2 == 0
        made = list(blocks)
        for i in range(16):
            if i & step:
                continue
            first, second = blocks[i], blocks[i + step]
            made[i] = jnp.where(low, first, pltpu.roll(second, 8 * step, 1))
            made[i + step] = jnp.where(low, pltpu.roll(first, N - 8 * step, 1), second)
        blocks = made
    return blocks


def kernel(
    density, factors, t_z, t_y, t_x, t_xb, t_yb, t_zb, out,
    d_ref, f_ref, z_ref, y_ref, x_ref, xb_ref, yb_ref, zb_ref,
    sa, sb, rf, sr, rb, pb, rows_ref, wide_ref, kernel_ref,
    load, send, recv,
):
    px, py = lax.axis_index("px"), lax.axis_index("py")
    core, y_chip = lax.rem(px, 2), lax.div(px, 2)
    other = 1 - core
    chip = py * ROWS_Y + y_chip
    partner = {"px": px + 1 - 2 * core}

    def peer(offset):
        to = lax.rem(chip + offset, CHIPS)
        return to, {"px": lax.rem(to, ROWS_Y) * 2 + core, "py": lax.div(to, ROWS_Y)}

    barrier = pltpu.get_barrier_semaphore()
    pl.semaphore_signal(barrier, inc=1, device_id=partner, device_id_type=MESH)
    for offset in ORDER:
        pl.semaphore_signal(barrier, inc=1, device_id=peer(offset)[1], device_id_type=MESH)

    loads = [
        pltpu.make_async_copy(src, dst, load.at[i])
        for i, (src, dst) in enumerate(
            [
                (density, d_ref), (t_z, z_ref), (factors.at[:, :, pl.ds(0, N)], f_ref), (t_y, y_ref),
                (t_x, x_ref), (t_xb, xb_ref), (t_yb, yb_ref), (t_zb, zb_ref),
            ]
        )
    ]
    for copy in loads:
        copy.start()
    loads[0].wait()
    loads[1].wait()
    for r in range(2):
        high, low = split(d_ref[r].reshape(N, N))
        both = jnp.concatenate([high, low], 1)
        for owner, to in ((core, sb.at[core, r]), (other, sa.at[r])):
            part = dot(z_ref[owner, :, : 2 * N], both, ((1,), (1,)))
            part += dot(z_ref[owner, :, 2 * N :], high, ((1,), (1,)))
            to[...] = part
    loads[2].wait()
    frequency = core * CHIPS + chip
    lane = lax.broadcasted_iota(jnp.int32, f_ref.shape[1:], 1)
    scale = jnp.sum(jnp.where(lane == frequency, f_ref[2], 0.0), axis=1, keepdims=True)
    kernel_ref[...] = lax.dot_general(
        f_ref[0] * scale, f_ref[1], (((0,), (0,)), ((), ())),
        precision=lax.Precision.HIGHEST, preferred_element_type=F32,
    )
    for copy in loads[3:]:
        copy.wait()

    pl.semaphore_wait(barrier, CHIPS)

    def pair(src, dst, i):
        return pltpu.make_async_remote_copy(
            src_ref=src, dst_ref=dst, send_sem=send.at[i], recv_sem=recv.at[i],
            device_id=partner, device_id_type=MESH,
        )

    def scatter(src, dst, i):
        pltpu.make_async_copy(src(chip), dst, recv.at[i]).start()
        for offset in ORDER:
            to, device = peer(offset)
            pltpu.make_async_remote_copy(
                src_ref=src(to), dst_ref=dst, send_sem=send.at[i], recv_sem=recv.at[i],
                device_id=device, device_id_type=MESH,
            ).start()

    def arrived(whole, i):
        pltpu.make_async_copy(whole, whole, recv.at[i]).wait()

    firsts = [pair(sa.at[r], sb.at[core, r], r) for r in range(2)]
    for copy in firsts:
        copy.start()
    sb5 = sb.reshape(2, 2, CHIPS, 2, N)
    rf5 = rf.reshape(2, CHIPS, 2, 2, N)
    sr5 = sr.reshape(2, CHIPS, 2, 2, N)
    rb5 = rb.reshape(2, 2, CHIPS, 2, N)
    for r in range(2):
        firsts[r].wait_recv()
        scatter(lambda to: sb5.at[:, r, to], rf5.at[r, chip], 2 + r)

    plane = kernel_ref[...]
    wide_plane = jnp.concatenate([plane, plane], 1)
    for r in range(2):
        arrived(rf.at[r], 2 + r)
        for h in range(2):
            blocks = swap([rf[r, pl.ds(16 * i + 8 * h, 8), :] for i in range(16)])
            for i in range(16):
                rows_ref[pl.ds(16 * i + 8 * h, 8), :] = blocks[i]
        high, low = split(rows_ref[...])
        wide = dot(jnp.concatenate([high, low], 1), y_ref[: 2 * N, :]) + dot(high, y_ref[2 * N :, :])
        for half in range(2):
            wide_ref[half] = wide[:, half * N : (half + 1) * N]
        for part in range(2):
            wide = [wide_ref[half, pl.ds(part, N, stride=2), :] for half in range(2)]
            high, low = split(jnp.concatenate(wide, 1))
            both = jnp.concatenate([high, low], 0)
            halves = []
            for half in range(2):
                rows = slice(half * N, (half + 1) * N)
                freq = dot(x_ref[rows, : 2 * N], both) + dot(x_ref[rows, 2 * N :], high)
                halves.append(split(freq * wide_plane))
            high = jnp.concatenate([halves[0][0], halves[1][0]], 0)
            low = jnp.concatenate([halves[0][1], halves[1][1]], 0)
            mixed = dot(xb_ref[:N, :], high) + dot(xb_ref[:N, :], low) + dot(xb_ref[N:, :], high)
            high, low = split(mixed)
            twice = dot(high, yb_ref[...])
            rows_ref[pl.ds(part, N, stride=2), :] = twice[:, :N] + twice[:, N:] + dot(low, yb_ref[:, :N])
        for h in range(2):
            blocks = swap([rows_ref[pl.ds(16 * i + 8 * h, 8), :] for i in range(16)])
            for i in range(16):
                sr[r, pl.ds(16 * i + 8 * h, 8), :] = blocks[i]
        scatter(lambda to: sr5.at[r, to], rb5.at[:, r, chip], 4 + r)

    lasts = [pair(rb.at[other, r], pb.at[r], 6 + r) for r in range(2)]
    for r in range(2):
        arrived(rb.at[:, r], 4 + r)
        lasts[r].start()
        high, low = split(rb[core, r])
        twice = dot(high, zb_ref[core], ((0,), (0,)))
        field = twice[:, :N] + twice[:, N:] + dot(low, zb_ref[core, :, :N], ((0,), (0,)))
        lasts[r].wait_recv()
        high, low = split(pb[r])
        twice = dot(high, zb_ref[other], ((0,), (0,)))
        field += twice[:, :N] + twice[:, N:] + dot(low, zb_ref[other, :, :N], ((0,), (0,)))
        out[r] = field.reshape(16, 8, N)
    for copy in firsts + lasts:
        copy.wait_send()
    for i in range(2, 6):
        some = rf5.at[0, pl.ds(0, CHIPS - 1)]
        pltpu.make_async_copy(some, some, send.at[i]).wait()


def body(density, kernel_factors):
    made = tables()
    held = [pltpu.VMEM(density.shape, F32), pltpu.VMEM(kernel_factors.shape[:2] + (N,), F32)]
    held += [pltpu.VMEM(table.shape, BF16) for table in made]
    scratch = [
        pltpu.VMEM((2, N, N), F32),
        pltpu.VMEM((2, 2, N, N), F32),
        pltpu.VMEM((2, 2 * N, N), F32),
        pltpu.VMEM((2, 2 * N, N), F32),
        pltpu.VMEM((2, 2, N, N), F32),
        pltpu.VMEM((2, N, N), F32),
        pltpu.VMEM((2 * N, N), F32),
        pltpu.VMEM((2, 2 * N, N), F32),
        pltpu.VMEM((N, N), F32),
        pltpu.SemaphoreType.DMA((8,)),
        pltpu.SemaphoreType.DMA((8,)),
        pltpu.SemaphoreType.DMA((8,)),
    ]
    return pl.pallas_call(
        kernel,
        out_shape=jax.ShapeDtypeStruct(density.shape, F32),
        in_specs=[pl.BlockSpec(memory_space=pl.ANY)] * (2 + len(made)),
        out_specs=pl.BlockSpec(memory_space=pltpu.VMEM),
        scratch_shapes=held + scratch,
        compiler_params=pltpu.CompilerParams(collective_id=0, has_side_effects=True),
        name="solve",
    )(density, kernel_factors, *[jnp.asarray(table) for table in made])


def solution(mesh):
    return jax.shard_map(
        body,
        mesh=mesh,
        in_specs=(P("rep", "px", "py", None), P()),
        out_specs=P("rep", "px", "py", None),
        check_vma=False,
    )
```

```python
import functools

import jax
import jax.numpy as jnp
import numpy as np
from jax import lax
from jax.experimental import pallas as pl
from jax.experimental.pallas import tpu as pltpu
from jax.sharding import PartitionSpec as P

MESH = pl.DeviceIdType.MESH
N = 128
CHIPS = 64
ROWS_Y = 4
F32, BF16 = jnp.float32, jnp.bfloat16
PARTS = 4
FIRST = 0


def order():
    steps = [(y, z, x) for y in (0, 1, 3, 2) for x in (0, 1) for z in (0, 1, 7, 2, 6, 3, 5, 4) if y or x or z]
    steps = [steps[i] for i in np.random.RandomState(0).permutation(len(steps))]
    return sorted(steps, key=lambda s: -(min(s[0], 4 - s[0]) + min(s[1], 8 - s[1]) + s[2]))


ORDER = order()


def pieces(table):
    table = np.asarray(table, np.float64).astype(np.float32)
    high = table.astype(BF16)
    low = (table - high.astype(np.float32)).astype(BF16)
    return high, low


def tables():
    k, n = np.arange(N), np.arange(N)
    angle = (k[:, None] * n[None, :] % (2 * N)) * (np.pi / N)
    cos, sin = np.cos(angle), np.sin(angle)
    weight = np.where(k == 0, 1.0, 2.0)[:, None] / (2 * N)
    by_owner = np.stack([cos, sin], 0).reshape(2, 2, CHIPS, N).swapaxes(0, 1).reshape(2, 2 * CHIPS, N)
    by_owner_back = np.stack([cos * weight, sin * weight], 0).reshape(2, 2, CHIPS, N).swapaxes(0, 1).reshape(2, 2 * CHIPS, N)
    plain = np.concatenate([cos, sin], 0)
    back = np.concatenate([cos * weight, sin * weight], 0)
    cells = np.arange(N).reshape(8, 16).T.reshape(-1)
    out = []
    high, low = pieces(by_owner)
    out.append(np.concatenate([high, high, low], 2))
    high, low = pieces(plain.T)
    out.append(np.concatenate([high, high, low], 0))
    high, low = pieces(plain[:, cells])
    out.append(np.concatenate([high, high, low], 1))
    high, low = pieces(back[:, cells].T)
    out.append(np.concatenate([high, low], 0))
    high, low = pieces(back)
    out.append(np.concatenate([high, low], 1))
    high, low = pieces(by_owner_back)
    out.append(np.concatenate([high, low], 2))
    return out


def split(value):
    high = value.astype(BF16)
    return high, (value - high.astype(F32)).astype(BF16)


def dot(a, b, dims=((1,), (0,))):
    return lax.dot_general(a, b, (dims, ((), ())), preferred_element_type=F32)


def swap(blocks):
    group = lax.broadcasted_iota(jnp.int32, (8, N), 1) // 8
    for bit in range(4):
        step = 1 << bit
        low = (group // step) % 2 == 0
        made = list(blocks)
        for i in range(16):
            if i & step:
                continue
            first, second = blocks[i], blocks[i + step]
            made[i] = jnp.where(low, first, pltpu.roll(second, 8 * step, 1))
            made[i + step] = jnp.where(low, pltpu.roll(first, N - 8 * step, 1), second)
        blocks = made
    return blocks


def kernel(
    density, factors, t_z, t_y, t_x, t_xb, t_yb, t_zb, out,
    d_ref, f_ref, z_ref, y_ref, x_ref, xb_ref, yb_ref, zb_ref,
    sa, sb, rf, sr, rb, pb, kernel_ref,
    load, send, recv,
):
    px, py = lax.axis_index("px"), lax.axis_index("py")
    core, y_chip = lax.rem(px, 2), lax.div(px, 2)
    x_chip, z_chip = lax.rem(py, 2), lax.div(py, 2)
    other = 1 - core
    chip = py * ROWS_Y + y_chip
    partner = {"px": px + 1 - 2 * core}
    ys = [lax.rem(y_chip + i, 4) for i in range(4)]
    zs = [lax.rem(z_chip + i, 8) for i in range(8)]
    xs = [x_chip, 1 - x_chip]
    peers = []
    for y, z, x in ORDER:
        to = zs[z] * 2 + xs[x]
        peers.append((to * ROWS_Y + ys[y], {"px": ys[y] * 2 + core, "py": to}))

    barrier = pltpu.get_barrier_semaphore()
    for _, device in peers:
        pl.semaphore_signal(barrier, inc=1, device_id=device, device_id_type=MESH)
    pl.semaphore_signal(barrier, inc=1, device_id=partner, device_id_type=MESH)

    loads = [
        pltpu.make_async_copy(src, dst, load.at[i])
        for i, (src, dst) in enumerate(
            [
                (density, d_ref), (t_z, z_ref), (factors.at[:, :, pl.ds(0, N)], f_ref), (t_y, y_ref),
                (t_x, x_ref), (t_xb, xb_ref), (t_yb, yb_ref), (t_zb, zb_ref),
            ]
        )
    ]
    for copy in loads:
        copy.start()
    loads[0].wait()
    loads[1].wait()
    for r in range(2):
        high, low = split(d_ref[r].reshape(N, N))
        both = jnp.concatenate([high, low], 1)
        for owner, mine in ((core, True), (other, False)):
            part = dot(z_ref[owner, :, : 2 * N], both, ((1,), (1,)))
            part += dot(z_ref[owner, :, 2 * N :], high, ((1,), (1,)))
            for i in range(2):
                rows = part[i * CHIPS : (i + 1) * CHIPS]
                if mine:
                    sb[2 * r + i, core] = rows
                else:
                    sa[2 * r + i] = rows
    loads[2].wait()
    frequency = core * CHIPS + chip
    lane = lax.broadcasted_iota(jnp.int32, f_ref.shape[1:], 1)
    scale = jnp.sum(jnp.where(lane == frequency, f_ref[2], 0.0), axis=1, keepdims=True)
    kernel_ref[...] = lax.dot_general(
        f_ref[0] * scale, f_ref[1], (((0,), (0,)), ((), ())),
        precision=lax.Precision.HIGHEST, preferred_element_type=F32,
    )
    for copy in loads[3:]:
        copy.wait()

    pl.semaphore_wait(barrier, CHIPS)

    def pair(src, dst, i):
        return pltpu.make_async_remote_copy(
            src_ref=src, dst_ref=dst, send_sem=send.at[i], recv_sem=recv.at[i],
            device_id=partner, device_id_type=MESH,
        )

    def scatter(src, dst, i):
        made = [pltpu.make_async_copy(src(chip), dst, recv.at[i])]
        for to, device in peers:
            made.append(
                pltpu.make_async_remote_copy(
                    src_ref=src(to), dst_ref=dst, send_sem=send.at[i], recv_sem=recv.at[i],
                    device_id=device, device_id_type=MESH,
                )
            )
        return made[1:] + made[:1]

    def arrived(whole, i):
        pltpu.make_async_copy(whole, whole, recv.at[i]).wait()

    firsts = [pair(sa.at[q], sb.at[q, core], q) for q in range(PARTS)]
    for copy in firsts:
        copy.start()
    sb6 = sb.reshape(PARTS, 2, CHIPS, 1, N)
    rf6 = rf.reshape(PARTS, CHIPS, 2, 1, N)
    sr6 = sr.reshape(PARTS, CHIPS, 2, 1, N)
    rb6 = rb.reshape(PARTS, 2, CHIPS, 1, N)
    for q in range(PARTS):
        firsts[q].wait_recv()
        for copy in scatter(lambda to: sb6.at[q, :, to], rf6.at[q, chip], PARTS + q):
            copy.start()

    waiting = []

    def emit(count):
        for _ in range(min(count, len(waiting))):
            waiting.pop(0).start()

    for q in range(PARTS):
        emit(FIRST)
        arrived(rf.at[q], PARTS + q)
        blocks = swap([rf[q, pl.ds(8 * i, 8), :] for i in range(16)])
        emit(16)
        high, low = split(jnp.concatenate(blocks, 0))
        wide = dot(jnp.concatenate([high, low], 1), y_ref[: 2 * N, :]) + dot(high, y_ref[2 * N :, :])
        emit(16)
        high, low = split(wide)
        both = jnp.concatenate([high, low], 0)
        plane = kernel_ref[...]
        wide_plane = jnp.concatenate([plane, plane], 1)
        halves = []
        for half in range(2):
            rows = slice(half * N, (half + 1) * N)
            freq = dot(x_ref[rows, : 2 * N], both) + dot(x_ref[rows, 2 * N :], high)
            halves.append(split(freq * wide_plane))
            emit(16)
        high = jnp.concatenate([halves[0][0], halves[1][0]], 0)
        low = jnp.concatenate([halves[0][1], halves[1][1]], 0)
        mixed = dot(xb_ref[:N, :], high) + dot(xb_ref[:N, :], low) + dot(xb_ref[N:, :], high)
        emit(CHIPS)
        high, low = split(mixed)
        twice = dot(high, yb_ref[...])
        cells = twice[:, :N] + twice[:, N:] + dot(low, yb_ref[:, :N])
        blocks = swap([cells[8 * i : 8 * i + 8] for i in range(16)])
        for i in range(16):
            sr[q, pl.ds(8 * i, 8), :] = blocks[i]
        waiting += scatter(lambda to, q=q: sr6.at[q, to], rb6.at[q, :, chip], 2 * PARTS + q)
    emit(CHIPS)

    lasts = [pair(rb.at[q, other], pb.at[q], 3 * PARTS + q) for q in range(PARTS)]
    for q in range(PARTS):
        arrived(rb.at[q], 2 * PARTS + q)
        lasts[q].start()
        if q % 2 == 0:
            continue
        r = q // 2
        field = jnp.zeros((N, N), F32)
        for owner, mine in ((core, True), (other, False)):
            if not mine:
                lasts[q - 1].wait_recv()
                lasts[q].wait_recv()
            pieces_of = [rb[i, core] if mine else pb[i] for i in (q - 1, q)]
            high, low = split(jnp.concatenate(pieces_of, 0))
            twice = dot(high, zb_ref[owner], ((0,), (0,)))
            field += twice[:, :N] + twice[:, N:] + dot(low, zb_ref[owner, :, :N], ((0,), (0,)))
        out[r] = field.reshape(16, 8, N)
    for copy in firsts + lasts:
        copy.wait_send()
    for i in range(PARTS, 3 * PARTS):
        some = rf6.at[0, pl.ds(0, CHIPS - 1)]
        pltpu.make_async_copy(some, some, send.at[i]).wait()


def body(density, kernel_factors):
    made = tables()
    held = [pltpu.VMEM(density.shape, F32), pltpu.VMEM(kernel_factors.shape[:2] + (N,), F32)]
    held += [pltpu.VMEM(table.shape, BF16) for table in made]
    scratch = [
        pltpu.VMEM((PARTS, CHIPS, N), F32),
        pltpu.VMEM((PARTS, 2, CHIPS, N), F32),
        pltpu.VMEM((PARTS, N, N), F32),
        pltpu.VMEM((PARTS, N, N), F32),
        pltpu.VMEM((PARTS, 2, CHIPS, N), F32),
        pltpu.VMEM((PARTS, CHIPS, N), F32),
        pltpu.VMEM((N, N), F32),
        pltpu.SemaphoreType.DMA((8,)),
        pltpu.SemaphoreType.DMA((4 * PARTS,)),
        pltpu.SemaphoreType.DMA((4 * PARTS,)),
    ]
    return pl.pallas_call(
        kernel,
        out_shape=jax.ShapeDtypeStruct(density.shape, F32),
        in_specs=[pl.BlockSpec(memory_space=pl.ANY)] * (2 + len(made)),
        out_specs=pl.BlockSpec(memory_space=pltpu.VMEM),
        scratch_shapes=held + scratch,
        compiler_params=pltpu.CompilerParams(collective_id=0, has_side_effects=True),
        name="solve",
    )(density, kernel_factors, *[jnp.asarray(table) for table in made])


def solution(mesh):
    return jax.shard_map(
        body,
        mesh=mesh,
        in_specs=(P("rep", "px", "py", None), P()),
        out_specs=P("rep", "px", "py", None),
        check_vma=False,
    )
```

```python
import functools

import jax
import jax.numpy as jnp
import numpy as np
from jax import lax
from jax.experimental import pallas as pl
from jax.experimental.pallas import tpu as pltpu
from jax.sharding import PartitionSpec as P

MESH = pl.DeviceIdType.MESH
N = 128
CHIPS = 64
ROWS_Y = 4
F32, BF16 = jnp.float32, jnp.bfloat16
PARTS = 4
OUT = ((0, 1), (1, 1), (2, 1), (3, 1))
BACK = ((0, 1), (1, 1), (2, 1), (3, 1))
DIRECT = (3,)
PIECE = (0, 16, 16, 16, 16, 128)


def order():
    steps = [(y, z, x) for y in (0, 1, 3, 2) for x in (0, 1) for z in (0, 1, 7, 2, 6, 3, 5, 4) if y or x or z]
    steps = [steps[i] for i in np.random.RandomState(0).permutation(len(steps))]
    return sorted(steps, key=lambda s: -(min(s[0], 4 - s[0]) + min(s[1], 8 - s[1]) + s[2]))


ORDER = order()


def pieces(table):
    table = np.asarray(table, np.float64).astype(np.float32)
    high = table.astype(BF16)
    low = (table - high.astype(np.float32)).astype(BF16)
    return high, low


def tables():
    k, n = np.arange(N), np.arange(N)
    angle = (k[:, None] * n[None, :] % (2 * N)) * (np.pi / N)
    cos, sin = np.cos(angle), np.sin(angle)
    weight = np.where(k == 0, 1.0, 2.0)[:, None] / (2 * N)
    by_owner = np.stack([cos, sin], 0).reshape(2, 2, CHIPS, N).swapaxes(0, 1).reshape(2, 2 * CHIPS, N)
    by_owner_back = np.stack([cos * weight, sin * weight], 0).reshape(2, 2, CHIPS, N)
    plain = np.concatenate([cos, sin], 0)
    back = np.concatenate([cos * weight, sin * weight], 0)
    cells = np.arange(N).reshape(8, 16).T.reshape(-1)
    out = []
    high, low = pieces(by_owner)
    out.append(np.concatenate([high, high, low], 2))
    high, low = pieces(plain.T)
    out.append(np.concatenate([high, high, low], 0))
    high, low = pieces(plain[:, cells])
    out.append(np.concatenate([high, high, low], 1))
    high, low = pieces(back[:, cells].T)
    out.append(np.concatenate([high, low], 0))
    high, low = pieces(back)
    out.append(np.concatenate([high, low], 1))
    high, low = pieces(by_owner_back)
    out.append(np.concatenate([high, low], 3))
    return out


def split(value):
    high = value.astype(BF16)
    return high, (value - high.astype(F32)).astype(BF16)


def dot(a, b, dims=((1,), (0,))):
    return lax.dot_general(a, b, (dims, ((), ())), preferred_element_type=F32)


def swap(blocks):
    group = lax.broadcasted_iota(jnp.int32, (8, N), 1) // 8
    for bit in range(4):
        step = 1 << bit
        low = (group // step) % 2 == 0
        made = list(blocks)
        for i in range(16):
            if i & step:
                continue
            first, second = blocks[i], blocks[i + step]
            made[i] = jnp.where(low, first, pltpu.roll(second, 8 * step, 1))
            made[i + step] = jnp.where(low, pltpu.roll(first, N - 8 * step, 1), second)
        blocks = made
    return blocks


def kernel(
    density, factors, t_z, t_y, t_x, t_xb, t_yb, t_zb, out,
    d_ref, f_ref, z_ref, y_ref, x_ref, xb_ref, yb_ref, zb_ref,
    sa, sb, rf, sr, rb, pb, kernel_ref,
    load, send, recv,
):
    px, py = lax.axis_index("px"), lax.axis_index("py")
    core, y_chip = lax.rem(px, 2), lax.div(px, 2)
    x_chip, z_chip = lax.rem(py, 2), lax.div(py, 2)
    other = 1 - core
    chip = py * ROWS_Y + y_chip
    partner = {"px": px + 1 - 2 * core}
    ys = [lax.rem(y_chip + i, 4) for i in range(4)]
    zs = [lax.rem(z_chip + i, 8) for i in range(8)]
    xs = [x_chip, 1 - x_chip]
    peers = []
    for y, z, x in ORDER:
        to = zs[z] * 2 + xs[x]
        peers.append((to * ROWS_Y + ys[y], {"px": ys[y] * 2 + core, "py": to}))

    barrier = pltpu.get_barrier_semaphore()
    for _, device in peers:
        pl.semaphore_signal(barrier, inc=1, device_id=device, device_id_type=MESH)
    pl.semaphore_signal(barrier, inc=1, device_id=partner, device_id_type=MESH)

    loads = [
        pltpu.make_async_copy(src, dst, load.at[i])
        for i, (src, dst) in enumerate(
            [
                (density, d_ref), (t_z, z_ref), (factors.at[:, :, pl.ds(0, N)], f_ref), (t_y, y_ref),
                (t_x, x_ref), (t_xb, xb_ref), (t_yb, yb_ref), (t_zb, zb_ref),
            ]
        )
    ]
    for copy in loads:
        copy.start()
    loads[0].wait()
    loads[1].wait()
    for r in range(2):
        high, low = split(d_ref[r].reshape(N, N))
        both = jnp.concatenate([high, low], 1)
        for owner, mine in ((core, True), (other, False)):
            part = dot(z_ref[owner, :, : 2 * N], both, ((1,), (1,)))
            part += dot(z_ref[owner, :, 2 * N :], high, ((1,), (1,)))
            for i in range(2):
                rows = part[i * CHIPS : (i + 1) * CHIPS]
                if mine:
                    sb[2 * r + i, core] = rows
                else:
                    sa[2 * r + i] = rows
    loads[2].wait()
    frequency = core * CHIPS + chip
    lane = lax.broadcasted_iota(jnp.int32, f_ref.shape[1:], 1)
    scale = jnp.sum(jnp.where(lane == frequency, f_ref[2], 0.0), axis=1, keepdims=True)
    kernel_ref[...] = lax.dot_general(
        f_ref[0] * scale, f_ref[1], (((0,), (0,)), ((), ())),
        precision=lax.Precision.HIGHEST, preferred_element_type=F32,
    )
    for copy in loads[3:]:
        copy.wait()

    pl.semaphore_wait(barrier, CHIPS)

    def pair(src, dst, i):
        return pltpu.make_async_remote_copy(
            src_ref=src, dst_ref=dst, send_sem=send.at[i], recv_sem=recv.at[i],
            device_id=partner, device_id_type=MESH,
        )

    def scatter(src, dst, i):
        made = []
        for to, device in peers:
            made.append(
                pltpu.make_async_remote_copy(
                    src_ref=src(to), dst_ref=dst, send_sem=send.at[i], recv_sem=recv.at[i],
                    device_id=device, device_id_type=MESH,
                )
            )
        return made + [pltpu.make_async_copy(src(chip), dst, recv.at[i])]

    def arrived(whole, i):
        pltpu.make_async_copy(whole, whole, recv.at[i]).wait()

    sb6 = sb.reshape(PARTS, 2, CHIPS, 1, N)
    rf6 = rf.reshape(PARTS, CHIPS, 2, 1, N)
    sr6 = sr.reshape(PARTS, CHIPS, 2, 1, N)
    rb6 = rb.reshape(PARTS, 2, CHIPS, 1, N)
    sent = []

    def drain(whole, i):
        sent.append((whole, i))

    firsts = [pair(sa.at[pl.ds(q, n)], sb.at[pl.ds(q, n), core], q) for q, n in OUT]
    for copy in firsts:
        copy.start()
    for i, (q, n) in enumerate(OUT):
        firsts[i].wait_recv()
        for copy in scatter(lambda to: sb6.at[pl.ds(q, n), :, to], rf6.at[pl.ds(q, n), chip], PARTS + q):
            copy.start()
        drain(rf6.at[pl.ds(q, n), pl.ds(0, CHIPS - 1)], PARTS + q)

    waiting = []

    def emit(point):
        for _ in range(min(PIECE[point], len(waiting))):
            waiting.pop(0).start()

    for q in range(PARTS):
        emit(0)
        for start, n in OUT:
            if start == q:
                arrived(rf.at[pl.ds(q, n)], PARTS + q)
        blocks = swap([rf[q, pl.ds(8 * i, 8), :] for i in range(16)])
        emit(1)
        high, low = split(jnp.concatenate(blocks, 0))
        wide = dot(jnp.concatenate([high, low], 1), y_ref[: 2 * N, :]) + dot(high, y_ref[2 * N :, :])
        emit(2)
        high, low = split(wide)
        both = jnp.concatenate([high, low], 0)
        plane = kernel_ref[...]
        wide_plane = jnp.concatenate([plane, plane], 1)
        halves = []
        for half in range(2):
            rows = slice(half * N, (half + 1) * N)
            freq = dot(x_ref[rows, : 2 * N], both) + dot(x_ref[rows, 2 * N :], high)
            halves.append(split(freq * wide_plane))
            emit(3 + half)
        high = jnp.concatenate([halves[0][0], halves[1][0]], 0)
        low = jnp.concatenate([halves[0][1], halves[1][1]], 0)
        mixed = dot(xb_ref[:N, :], high) + dot(xb_ref[:N, :], low) + dot(xb_ref[N:, :], high)
        emit(5)
        high, low = split(mixed)
        twice = dot(high, yb_ref[...])
        cells = twice[:, :N] + twice[:, N:] + dot(low, yb_ref[:, :N])
        blocks = swap([cells[8 * i : 8 * i + 8] for i in range(16)])
        for i in range(16):
            sr[q, pl.ds(8 * i, 8), :] = blocks[i]
        if q in DIRECT:
            flag = 2 * PARTS + q
            for to, device in peers:
                for core_to in (core, other):
                    waiting.append(
                        pltpu.make_async_remote_copy(
                            src_ref=sr6.at[q, to, core_to], dst_ref=rb6.at[q, core, chip],
                            send_sem=send.at[flag], recv_sem=recv.at[flag],
                            device_id={"px": device["px"] + core_to - core, "py": device["py"]}, device_id_type=MESH,
                        )
                    )
            waiting.append(pair(sr6.at[q, chip, other], rb6.at[q, core, chip], flag))
            waiting.append(pltpu.make_async_copy(sr6.at[q, chip, core], rb6.at[q, core, chip], recv.at[flag]))
            drain(rf.reshape(PARTS, N, 1, N).at[q, pl.ds(0, N - 1)], flag)
        else:
            for start, n in BACK:
                if start + n - 1 == q:
                    some = pl.ds(start, n)
                    waiting += scatter(lambda to, some=some: sr6.at[some, to], rb6.at[some, :, chip], 2 * PARTS + start)
                    drain(rf6.at[some, pl.ds(0, CHIPS - 1)], 2 * PARTS + start)
    for copy in waiting:
        copy.start()

    def back(rows, table):
        high, low = split(rows)
        twice = dot(high, table, ((0,), (0,)))
        return twice[:, :N] + twice[:, N:] + dot(low, table[:, :N], ((0,), (0,)))

    lasts, fields = {}, [None, None]

    def add(r, part):
        fields[r] = part if fields[r] is None else fields[r] + part

    groups = [g for g in BACK if g[0] not in DIRECT]
    for start, n in groups:
        arrived(rb.at[pl.ds(start, n)], 2 * PARTS + start)
        lasts[start] = pair(rb.at[pl.ds(start, n), other], pb.at[pl.ds(start, n)], 3 * PARTS + start)
        lasts[start].start()
    for start, n in groups:
        for q in range(start, start + n):
            add(q // 2, back(rb[q, core], zb_ref[q % 2, core]))
    for start, n in groups:
        lasts[start].wait_recv()
        for q in range(start, start + n):
            add(q // 2, back(pb[q], zb_ref[q % 2, other]))
    for q in range(PARTS):
        if q in DIRECT:
            arrived(rb.at[q], 2 * PARTS + q)
            add(q // 2, back(rb[q].reshape(N, N), zb_ref[q % 2].reshape(N, 2 * N)))
    for r in range(2):
        out[r] = fields[r].reshape(16, 8, N)
    for copy in firsts + list(lasts.values()):
        copy.wait_send()
    for whole, i in sent:
        pltpu.make_async_copy(whole, whole, send.at[i]).wait()


def body(density, kernel_factors):
    made = tables()
    held = [pltpu.VMEM(density.shape, F32), pltpu.VMEM(kernel_factors.shape[:2] + (N,), F32)]
    held += [pltpu.VMEM(table.shape, BF16) for table in made]
    scratch = [
        pltpu.VMEM((PARTS, CHIPS, N), F32),
        pltpu.VMEM((PARTS, 2, CHIPS, N), F32),
        pltpu.VMEM((PARTS, N, N), F32),
        pltpu.VMEM((PARTS, N, N), F32),
        pltpu.VMEM((PARTS, 2, CHIPS, N), F32),
        pltpu.VMEM((PARTS, CHIPS, N), F32),
        pltpu.VMEM((N, N), F32),
        pltpu.SemaphoreType.DMA((8,)),
        pltpu.SemaphoreType.DMA((4 * PARTS,)),
        pltpu.SemaphoreType.DMA((4 * PARTS,)),
    ]
    return pl.pallas_call(
        kernel,
        out_shape=pltpu.VMEM(density.shape, F32),
        in_specs=[pl.BlockSpec(memory_space=pl.ANY)] * (2 + len(made)),
        out_specs=pl.BlockSpec(memory_space=pltpu.VMEM),
        scratch_shapes=held + scratch,
        compiler_params=pltpu.CompilerParams(collective_id=0, has_side_effects=True),
        name="solve",
    )(density, kernel_factors, *[jnp.asarray(table) for table in made])


def solution(mesh):
    return jax.shard_map(
        body,
        mesh=mesh,
        in_specs=(P("rep", "px", "py", None), P()),
        out_specs=P("rep", "px", "py", None),
        check_vma=False,
    )
```

```python
import functools

import jax
import jax.numpy as jnp
import numpy as np
from jax import lax
from jax.experimental import pallas as pl
from jax.experimental.pallas import tpu as pltpu
from jax.sharding import PartitionSpec as P

MESH = pl.DeviceIdType.MESH
N = 128
CHIPS = 64
ROWS_Y = 4
F32, BF16 = jnp.float32, jnp.bfloat16
PARTS = 4
PIECE = (0, 24, 24, 24, 24, 24)


def order():
    steps = [(y, z, x) for y in (0, 1, 3, 2) for x in (0, 1) for z in (0, 1, 7, 2, 6, 3, 5, 4) if y or x or z]
    steps = [steps[i] for i in np.random.RandomState(0).permutation(len(steps))]
    return sorted(steps, key=lambda s: -hops(s))


def hops(s):
    return min(s[0], 4 - s[0]) + min(s[1], 8 - s[1]) + s[2]


ORDER = order()


def pieces(table):
    table = np.asarray(table, np.float64).astype(np.float32)
    high = table.astype(BF16)
    low = (table - high.astype(np.float32)).astype(BF16)
    return high, low


def tables():
    k, n = np.arange(N), np.arange(N)
    angle = (k[:, None] * n[None, :] % (2 * N)) * (np.pi / N)
    cos, sin = np.cos(angle), np.sin(angle)
    weight = np.where(k == 0, 1.0, 2.0)[:, None] / (2 * N)
    by_owner = np.stack([cos, sin], 0).reshape(2, 2, CHIPS, N).swapaxes(0, 1).reshape(2, 2 * CHIPS, N)
    by_owner_back = np.stack([cos * weight, sin * weight], 0).reshape(2, 2, CHIPS, N)
    plain = np.concatenate([cos, sin], 0)
    back = np.concatenate([cos * weight, sin * weight], 0)
    cells = np.arange(N).reshape(8, 16).T.reshape(-1)
    out = []
    high, low = pieces(by_owner)
    out.append(np.concatenate([high, high, low], 2))
    high, low = pieces(plain.T)
    out.append(np.concatenate([high, high, low], 0))
    high, low = pieces(plain[:, cells])
    out.append(np.concatenate([high, high, low], 1))
    high, low = pieces(back[:, cells].T)
    out.append(np.concatenate([high, low], 0))
    high, low = pieces(back)
    out.append(np.concatenate([high, low], 1))
    high, low = pieces(by_owner_back)
    out.append(np.concatenate([high, low], 3))
    return out


def split(value):
    high = value.astype(BF16)
    return high, (value - high.astype(F32)).astype(BF16)


def dot(a, b, dims=((1,), (0,))):
    return lax.dot_general(a, b, (dims, ((), ())), preferred_element_type=F32)


def swap(blocks):
    group = lax.broadcasted_iota(jnp.int32, (8, N), 1) // 8
    for bit in range(4):
        step = 1 << bit
        low = (group // step) % 2 == 0
        made = list(blocks)
        for i in range(16):
            if i & step:
                continue
            first, second = blocks[i], blocks[i + step]
            made[i] = jnp.where(low, first, pltpu.roll(second, 8 * step, 1))
            made[i + step] = jnp.where(low, pltpu.roll(first, N - 8 * step, 1), second)
        blocks = made
    return blocks


def kernel(
    density, factors, t_z, t_y, t_x, t_xb, t_yb, t_zb, out,
    d_ref, f_ref, z_ref, y_ref, x_ref, xb_ref, yb_ref, zb_ref,
    sa, sb, rf, sr, rb, kernel_ref,
    load, send, recv, ready,
):
    px, py = lax.axis_index("px"), lax.axis_index("py")
    core, y_chip = lax.rem(px, 2), lax.div(px, 2)
    x_chip, z_chip = lax.rem(py, 2), lax.div(py, 2)
    other = 1 - core
    chip = py * ROWS_Y + y_chip
    ys = [lax.rem(y_chip + i, 4) for i in range(4)]
    zs = [lax.rem(z_chip + i, 8) for i in range(8)]
    xs = [x_chip, 1 - x_chip]
    peers = []
    for y, z, x in ORDER:
        to = zs[z] * 2 + xs[x]
        peers.append((hops((y, z, x)), to * ROWS_Y + ys[y], ys[y] * 2, to))

    barrier = pltpu.get_barrier_semaphore()
    for _, _, to_px, to_py in peers:
        pl.semaphore_signal(barrier, inc=1, device_id={"px": to_px + core, "py": to_py}, device_id_type=MESH)
    pl.semaphore_signal(barrier, inc=1, device_id={"px": 2 * y_chip + other, "py": py}, device_id_type=MESH)

    loads = [
        pltpu.make_async_copy(src, dst, load.at[i])
        for i, (src, dst) in enumerate(
            [
                (density, d_ref), (t_z, z_ref), (factors.at[:, :, pl.ds(0, N)], f_ref), (t_y, y_ref),
                (t_x, x_ref), (t_xb, xb_ref), (t_yb, yb_ref), (t_zb, zb_ref),
            ]
        )
    ]
    for copy in loads:
        copy.start()
    loads[0].wait()
    loads[1].wait()
    for r in range(2):
        high, low = split(d_ref[r].reshape(N, N))
        both = jnp.concatenate([high, low], 1)
        for owner, mine in ((core, True), (other, False)):
            part = dot(z_ref[owner, :, : 2 * N], both, ((1,), (1,)))
            part += dot(z_ref[owner, :, 2 * N :], high, ((1,), (1,)))
            for i in range(2):
                rows = part[i * CHIPS : (i + 1) * CHIPS]
                if mine:
                    sb[2 * r + i, core] = rows
                else:
                    sa[2 * r + i] = rows
    loads[2].wait()
    frequency = core * CHIPS + chip
    lane = lax.broadcasted_iota(jnp.int32, f_ref.shape[1:], 1)
    scale = jnp.sum(jnp.where(lane == frequency, f_ref[2], 0.0), axis=1, keepdims=True)
    kernel_ref[...] = lax.dot_general(
        f_ref[0] * scale, f_ref[1], (((0,), (0,)), ((), ())),
        precision=lax.Precision.HIGHEST, preferred_element_type=F32,
    )
    for copy in loads[3:]:
        copy.wait()

    pl.semaphore_wait(barrier, CHIPS)

    def push(src, dst, i, to_px, to_py):
        return pltpu.make_async_remote_copy(
            src_ref=src, dst_ref=dst, send_sem=send.at[i], recv_sem=recv.at[i],
            device_id={"px": to_px, "py": to_py}, device_id_type=MESH,
        )

    def arrived(whole, i):
        pltpu.make_async_copy(whole, whole, recv.at[i]).wait()

    sb6 = sb.reshape(PARTS, 2, CHIPS, 1, N)
    rf6 = rf.reshape(PARTS, CHIPS, 2, 1, N)
    sr6 = sr.reshape(PARTS, CHIPS, 2, 1, N)
    rb6 = rb.reshape(PARTS, 2, CHIPS, 1, N)
    rows_of = rf.reshape(PARTS, N, 1, N)

    pl.semaphore_signal(ready, inc=1, device_id={"px": 2 * y_chip + other, "py": py}, device_id_type=MESH)
    between = push(sa.at[pl.ds(1, PARTS - 1)], sb.at[pl.ds(1, PARTS - 1), core], 0, 2 * y_chip + other, py)
    between.start()
    sa6 = sa.reshape(PARTS, CHIPS, 1, N)
    first = rf6.at[0, chip, core]
    for _, to, to_px, to_py in peers:
        push(sb6.at[0, core, to], first, 1, to_px + core, to_py).start()
    pl.semaphore_wait(ready, 1)
    for _, to, to_px, to_py in peers:
        push(sa6.at[0, to], first, 1, to_px + other, to_py).start()
    push(sa6.at[0, chip], first, 1, 2 * y_chip + other, py).start()
    pltpu.make_async_copy(sb6.at[0, core, chip], first, recv.at[1]).start()
    between.wait_recv()
    for q in range(1, PARTS):
        for _, to, to_px, to_py in peers:
            push(sb6.at[q, :, to], rf6.at[q, chip], 1 + q, to_px + core, to_py).start()
        pltpu.make_async_copy(sb6.at[q, :, chip], rf6.at[q, chip], recv.at[1 + q]).start()

    waiting = []

    def emit(point):
        for _ in range(min(PIECE[point], len(waiting))):
            waiting.pop(0)[1].start()

    for q in range(PARTS):
        emit(0)
        arrived(rf.at[q], 1 + q)
        blocks = swap([rf[q, pl.ds(8 * i, 8), :] for i in range(16)])
        emit(1)
        high, low = split(jnp.concatenate(blocks, 0))
        wide = dot(jnp.concatenate([high, low], 1), y_ref[: 2 * N, :]) + dot(high, y_ref[2 * N :, :])
        emit(2)
        high, low = split(wide)
        both = jnp.concatenate([high, low], 0)
        plane = kernel_ref[...]
        wide_plane = jnp.concatenate([plane, plane], 1)
        halves = []
        for half in range(2):
            rows = slice(half * N, (half + 1) * N)
            freq = dot(x_ref[rows, : 2 * N], both) + dot(x_ref[rows, 2 * N :], high)
            halves.append(split(freq * wide_plane))
            emit(3 + half)
        high = jnp.concatenate([halves[0][0], halves[1][0]], 0)
        low = jnp.concatenate([halves[0][1], halves[1][1]], 0)
        mixed = dot(xb_ref[:N, :], high) + dot(xb_ref[:N, :], low) + dot(xb_ref[N:, :], high)
        emit(5)
        high, low = split(mixed)
        twice = dot(high, yb_ref[...])
        cells = twice[:, :N] + twice[:, N:] + dot(low, yb_ref[:, :N])
        blocks = swap([cells[8 * i : 8 * i + 8] for i in range(16)])
        for i in range(16):
            sr[q, pl.ds(8 * i, 8), :] = blocks[i]
        flag = 1 + PARTS + q
        for far, to, to_px, to_py in peers:
            for core_to in (core, other):
                waiting.append((far, push(sr6.at[q, to, core_to], rb6.at[q, core, chip], flag, to_px + core_to, to_py)))
        waiting.append((0, push(sr6.at[q, chip, other], rb6.at[q, core, chip], flag, 2 * y_chip + other, py)))
        waiting.append((0, pltpu.make_async_copy(sr6.at[q, chip, core], rb6.at[q, core, chip], recv.at[flag])))
        waiting.sort(key=lambda pair: -pair[0])
    for _, copy in waiting:
        copy.start()

    def back(rows, table):
        high, low = split(rows)
        twice = dot(high, table, ((0,), (0,)))
        return twice[:, :N] + twice[:, N:] + dot(low, table[:, :N], ((0,), (0,)))

    for r in range(2):
        field = None
        for q in (2 * r, 2 * r + 1):
            arrived(rb.at[q], 1 + PARTS + q)
            part = back(rb[q].reshape(N, N), zb_ref[q % 2].reshape(N, 2 * N))
            field = part if field is None else field + part
        out[r] = field.reshape(16, 8, N)
    between.wait_send()
    for q in range(PARTS):
        out_of = rows_of.at[q, pl.ds(0, N - 1)] if q == 0 else rf6.at[q, pl.ds(0, CHIPS - 1)]
        for some, i in ((out_of, 1 + q), (rows_of.at[q, pl.ds(0, N - 1)], 1 + PARTS + q)):
            pltpu.make_async_copy(some, some, send.at[i]).wait()


def body(density, kernel_factors):
    made = tables()
    held = [pltpu.VMEM(density.shape, F32), pltpu.VMEM(kernel_factors.shape[:2] + (N,), F32)]
    held += [pltpu.VMEM(table.shape, BF16) for table in made]
    scratch = [
        pltpu.VMEM((PARTS, CHIPS, N), F32),
        pltpu.VMEM((PARTS, 2, CHIPS, N), F32),
        pltpu.VMEM((PARTS, N, N), F32),
        pltpu.VMEM((PARTS, N, N), F32),
        pltpu.VMEM((PARTS, 2, CHIPS, N), F32),
        pltpu.VMEM((N, N), F32),
        pltpu.SemaphoreType.DMA((8,)),
        pltpu.SemaphoreType.DMA((1 + 2 * PARTS,)),
        pltpu.SemaphoreType.DMA((1 + 2 * PARTS,)),
        pltpu.SemaphoreType.REGULAR,
    ]
    return pl.pallas_call(
        kernel,
        out_shape=pltpu.VMEM(density.shape, F32),
        in_specs=[pl.BlockSpec(memory_space=pl.ANY)] * (2 + len(made)),
        out_specs=pl.BlockSpec(memory_space=pltpu.VMEM),
        scratch_shapes=held + scratch,
        compiler_params=pltpu.CompilerParams(collective_id=0, has_side_effects=True),
        name="solve",
    )(density, kernel_factors, *[jnp.asarray(table) for table in made])


def solution(mesh):
    return jax.shard_map(
        body,
        mesh=mesh,
        in_specs=(P("rep", "px", "py", None), P()),
        out_specs=P("rep", "px", "py", None),
        check_vma=False,
    )
```
